32 devices in a mesh: dp: 8 (over z, x), mp: 4 (over y, core).
Axes of the slice: x: 2, y: 2, z: 4, core: 2. Of those that a mesh axis runs over, the one named last changes fastest.
Arguments:
- z_star: bfloat16 [8, 257, 1280], P('dp', None, 'mp'), may hold values from -24 to 24
- cotangent: float32 [8, 257, 1280], P('dp', None, 'mp'), may hold values from -6 to 6
- w_qkv: bfloat16 [3, 1280, 1280], P(None, None, 'mp'), may hold values from -1 to 1
- w_out: bfloat16 [1280, 1280], P('mp'), may hold values from -0.15625 to 0.15625
Outputs:
- implicit: float32 [8, 257, 1280], P('dp', None, 'mp')
- grad_qkv: float32 [3, 1280, 1280], P(None, 'dp', 'mp')
- grad_out: float32 [1280, 1280], P('mp', 'dp')
The draws below stay inside these ranges and needn't reach their ends.
All inputs are finite; a program needn't handle non-finite values.
Results may differ from the reference program's by a relative error of at most 0.0091.
Values may be sent and summed in bfloat16 or wider, within the bound.
A program may use at most 128 MiB of HBM per device.

```python
import math
import jax
import jax.numpy as jnp
from jax import lax

D = 1280
HEADS = 16
HD = 80
S = 257
IMG_DEV = 1
TERMS = 3
HH = 1280
IMAGES = 8
N_DP = 8


def boosted(key):
    shuffled = jax.random.permutation(jax.random.fold_in(key, 7), N_DP)
    owners = shuffled[jnp.arange(IMAGES) // IMG_DEV]
    blocks = jnp.arange(D) // (D // N_DP)
    return jnp.where(blocks[None, :] == owners[:, None], 3.0, 1.0).astype(jnp.float32)


def draw_z_star(key, part):
    scales = boosted(key)
    values = jnp.clip(jax.random.normal(jax.random.fold_in(key, 1), (IMAGES, S, D), jnp.float32), -6.0, 6.0)
    return (values * scales[:, None, :]).astype(jnp.bfloat16)


def draw_w_qkv(key, part):
    values = jnp.clip(jax.random.normal(jax.random.fold_in(key, 11), (3, D, HEADS * HD), jnp.float32), -6.0, 6.0) / math.sqrt(D)
    return values.astype(jnp.bfloat16)


def strengthened(values, own_key, source, target, shards_of, factor):
    owner, partner = [(jnp.arange(values.shape[dim]) // (values.shape[dim] // shards_of)).reshape([-1 if axis == dim else 1 for axis in range(values.ndim)]) for dim in (source, target)]
    chosen = jax.random.permutation(own_key, shards_of)[partner]
    strong = (owner == chosen) | (owner == (partner + shards_of // 2) % shards_of)
    return jnp.where(strong, factor * values, values)


def level_of(key, dims, shards, least, largest):
    def one(dim, parts):
        draws = jax.random.uniform(jax.random.fold_in(jax.random.fold_in(key, 6), dim), (parts,), jnp.float32, least / len(shards), largest / len(shards))
        return jnp.repeat(jnp.exp(draws), dims[dim] // parts).reshape((-1,) + (1,) * (len(dims) - dim - 1))

    gain = one(*shards[0])
    for cut in shards[1:]:
        gain = gain * one(*cut)
    return gain


def scatter_about(stream_key, shape, scale, bound, split=(), dtype=jnp.bfloat16):
    drawn = scale * jax.random.normal(stream_key, shape, jnp.float32)
    if split:
        drawn = drawn * level_of(stream_key, shape, split, -0.22, 0.18)
    return jnp.clip(drawn, -bound, bound).astype(dtype)


def bell_draw_with(key, shape, scale, reach, pieces, heavy, kind=jnp.bfloat16):
    values = scale * jax.random.normal(key, shape, jnp.float32)
    if pieces:
        values = values * level_of(key, shape, pieces, -0.22, 0.18)
    return jnp.clip(strengthened(values, jax.random.fold_in(key, 3), *heavy), -reach, reach).astype(kind)


def setup_inputs(seed: int = 0) -> dict:
    key_of = jax.random.split(jax.random.key(seed), 5)
    z_star = draw_z_star(jax.random.fold_in(key_of[4], 71), 0)
    cotangent = bell_draw_with(key_of[1], (IMAGES, S, D), 1.0, 6.0, ((0, 8), (2, 4)), (0, 2, 8, 2.0), jnp.float32)
    w_qkv = draw_w_qkv(jax.random.fold_in(key_of[4], 71), 0)
    w_out = scatter_about(key_of[3], (HH, D), HH ** -0.5, 0.15625, ((0, 4),))
    return dict(z_star=z_star, cotangent=cotangent, w_qkv=w_qkv, w_out=w_out)


epsilon = 1e-06

def layer_norm(z_block):
    values = z_block.astype(jnp.float32)
    centred = values - lax.optimization_barrier(jnp.mean(values, axis=-1, keepdims=True))
    inv_std = lax.rsqrt(lax.optimization_barrier(jnp.mean(centred * centred, axis=-1, keepdims=True)) + epsilon)
    return (centred * inv_std, inv_std)

def reference(z_star, cotangent, w_qkv, w_out):
    score_scale = HD ** (-0.5)
    features = HEADS * HD

    def one_block(running_grads, inputs):
        grad_q, grad_o = running_grads
        z_block, cot_block = inputs
        images, tokens, model_width = z_block.shape
        normal_f, inv_std = layer_norm(z_block)
        normal_b = normal_f.astype(jnp.bfloat16)
        flattened = normal_b.reshape(-1, model_width)

        def project(slot_index):
            result = jnp.dot(flattened, w_qkv[slot_index], preferred_element_type=jnp.float32)
            return result.astype(jnp.bfloat16).reshape(images, tokens, HEADS, HD)
        queries = project(0)
        key_vecs = project(1)
        val_vecs = project(2)
        scores = jnp.einsum('bqhe,bkhe->bhqk', queries.astype(jnp.float32), key_vecs.astype(jnp.float32)) * score_scale
        attn_probs = jax.nn.softmax(scores, axis=-1)
        probs_b = attn_probs.astype(jnp.bfloat16)
        attended = jnp.einsum('bhqk,bkhe->bqhe', probs_b.astype(jnp.float32), val_vecs.astype(jnp.float32))
        attended = attended.astype(jnp.bfloat16).reshape(-1, features)
        current = cot_block
        running = cot_block
        for term_index in range(TERMS):
            cot_b = current.astype(jnp.bfloat16).reshape(-1, model_width)
            att_grad = jnp.dot(cot_b, w_out.T, preferred_element_type=jnp.float32)
            att_grad = att_grad.astype(jnp.bfloat16).reshape(images, tokens, HEADS, HD)
            grad_o = grad_o + jnp.dot(attended.T, cot_b, preferred_element_type=jnp.float32)
            prob_grad = jnp.einsum('bqhe,bkhe->bhqk', att_grad.astype(jnp.float32), val_vecs.astype(jnp.float32))
            rowdot = lax.optimization_barrier(jnp.sum(attn_probs * prob_grad, axis=-1, keepdims=True))
            score_grad = (attn_probs * (prob_grad - rowdot) * score_scale).astype(jnp.bfloat16)
            q_grad = jnp.einsum('bhqk,bkhe->bqhe', score_grad.astype(jnp.float32), key_vecs.astype(jnp.float32)).astype(jnp.bfloat16)
            k_grad = jnp.einsum('bhqk,bqhe->bkhe', score_grad.astype(jnp.float32), queries.astype(jnp.float32)).astype(jnp.bfloat16)
            v_grad = jnp.einsum('bhqk,bqhe->bkhe', probs_b.astype(jnp.float32), att_grad.astype(jnp.float32)).astype(jnp.bfloat16)
            qkv_grads = [item.reshape(-1, features) for item in (q_grad, k_grad, v_grad)]
            grad_q = grad_q + jnp.stack([jnp.dot(flattened.T, item, preferred_element_type=jnp.float32) for item in qkv_grads])
            if term_index + 1 < TERMS:
                in_grad = jnp.dot(qkv_grads[0], w_qkv[0].T, preferred_element_type=jnp.float32)
                in_grad = in_grad + jnp.dot(qkv_grads[1], w_qkv[1].T, preferred_element_type=jnp.float32)
                in_grad = in_grad + jnp.dot(qkv_grads[2], w_qkv[2].T, preferred_element_type=jnp.float32)
                in_grad = in_grad.reshape(images, tokens, model_width)
                row_mean = lax.optimization_barrier(jnp.mean(in_grad, axis=-1, keepdims=True))
                row_dot = lax.optimization_barrier(jnp.mean(in_grad * normal_f, axis=-1, keepdims=True))
                current = (in_grad - row_mean - normal_f * row_dot) * inv_std
                running = running + current
        return ((grad_q, grad_o), running)
    blocks = IMAGES // IMG_DEV
    z_blocks = z_star.reshape(blocks, IMG_DEV, S, D)
    cot_blocks = cotangent.reshape(blocks, IMG_DEV, S, D)
    start = (jnp.zeros((3, D, features), jnp.float32), jnp.zeros((features, D), jnp.float32))
    (grad_q, grad_o), totals = lax.scan(one_block, start, (z_blocks, cot_blocks))
    factor = 1.0 / math.sqrt(IMAGES * S)
    return (totals.reshape(IMAGES, S, D), grad_q * factor, grad_o * factor)
```

```python
import functools
import math

import jax
import jax.numpy as jnp
from jax import lax
from jax.experimental import pallas as pl
from jax.experimental.pallas import tpu as pltpu
from jax.sharding import PartitionSpec as P

HD = 80
TERMS = 3
LANES = 128
MESH = pl.DeviceIdType.MESH


epsilon = 1e-06


def greet(axis, partners):
    barrier = pltpu.get_barrier_semaphore()
    for partner in partners:
        pl.semaphore_signal(barrier, inc=1, device_id={axis: partner}, device_id_type=MESH)
    pl.semaphore_wait(barrier, len(partners))


def remote(src, dst, send, recv, axis, target):
    return pltpu.make_async_remote_copy(
        src_ref=src, dst_ref=dst, send_sem=send, recv_sem=recv,
        device_id={axis: target}, device_id_type=MESH,
    )


def mp_partners():
    me = lax.axis_index("mp")
    core = lax.rem(me, 2)
    return me, core, me + 1 - 2 * core, lax.rem(me + 2, 4)


def gather_kernel(z_ref, cot_ref, nf_ref, nb_ref, inv_ref, cb_ref, cast, z_all, c_all, send, recv):
    me, core, other, across = mp_partners()
    narrow = z_ref.shape[1]
    cast[...] = cot_ref[...].astype(jnp.bfloat16)
    greet("mp", (other, across))
    copies = []
    for k, (src, held) in enumerate(((z_ref, z_all), (cast, c_all))):
        far = remote(src, held.at[me], send.at[k, 0], recv.at[k, 0], "mp", across)
        near = remote(src, held.at[me], send.at[k, 1], recv.at[k, 1], "mp", other)
        far.start()
        near.start()
        copies.append((far, near))

    def finish(k, src, held):
        far, near = copies[k]
        held[me] = src[...]
        far.wait_recv()
        passed = remote(
            held.at[across], held.at[across], send.at[k, 2], recv.at[k, 2], "mp", other
        )
        passed.start()
        near.wait_recv()
        passed.wait_recv()
        far.wait_send()
        near.wait_send()
        passed.wait_send()

    finish(0, z_ref, z_all)
    for s in range(4):
        nf_ref[:, s * narrow : (s + 1) * narrow] = z_all[s].astype(jnp.float32)
    values = nf_ref[...]
    centred = values - jnp.mean(values, axis=-1, keepdims=True)
    inv = lax.rsqrt(jnp.mean(centred * centred, axis=-1, keepdims=True) + epsilon)
    normal = centred * inv
    nf_ref[...] = normal
    nb_ref[...] = normal.astype(jnp.bfloat16)
    inv_ref[...] = inv
    finish(1, cast, c_all)
    for s in range(4):
        cb_ref[:, s * narrow : (s + 1) * narrow] = c_all[s]


def vmem(count):
    return [pl.BlockSpec(memory_space=pltpu.VMEM)] * count


def gather(z, cot):
    tokens, narrow = z.shape
    width = narrow * 4
    held = pltpu.VMEM((4, tokens, narrow), jnp.bfloat16)
    return pl.pallas_call(
        gather_kernel,
        name="gather_mp",
        out_shape=(
            jax.ShapeDtypeStruct((tokens, width), jnp.float32),
            jax.ShapeDtypeStruct((tokens, width), jnp.bfloat16),
            jax.ShapeDtypeStruct((tokens, 1), jnp.float32),
            jax.ShapeDtypeStruct((tokens, width), jnp.bfloat16),
        ),
        in_specs=vmem(2),
        out_specs=tuple(vmem(4)),
        scratch_shapes=[
            pltpu.VMEM((tokens, narrow), jnp.bfloat16),
            held,
            held,
            pltpu.SemaphoreType.DMA((2, 3)),
            pltpu.SemaphoreType.DMA((2, 3)),
        ],
        compiler_params=pltpu.CompilerParams(collective_id=0, has_side_effects=True),
    )(z, cot)


def reduce_kernel(last, part, nf, inv, cb, *refs):
    if last:
        ub_ref, term_ref, a_in, acc, b_out, b_in, c_out, c_in, total, send, recv = refs
    else:
        ub_ref, a_in, acc, b_out, b_in, c_out, c_in, total, send, recv = refs
    me, core, other, across = mp_partners()
    width = part.shape[1]
    half = width // 2
    pieces = half // LANES
    greet("mp", (other, across))

    def columns(which, j):
        return pl.ds(pl.multiple_of(which * half + j * LANES, LANES), LANES)

    first, second, third = [], [], []
    for j in range(pieces):
        copy = remote(
            part.at[:, columns(1 - core, j)], a_in.at[j], send.at[0, j], recv.at[0, j], "mp", other
        )
        copy.start()
        first.append(copy)
    for j in range(pieces):
        first[j].wait_recv()
        summed = part[:, columns(core, j)] + a_in[j]
        acc[j] = summed
        b_out[j] = summed.astype(jnp.bfloat16)
        copy = remote(b_out.at[j], b_in.at[j], send.at[1, j], recv.at[1, j], "mp", across)
        copy.start()
        second.append(copy)
    for j in range(pieces):
        second[j].wait_recv()
        summed = acc[j] + b_in[j].astype(jnp.float32)
        total[core * pieces + j] = summed
        c_out[j] = summed.astype(jnp.bfloat16)
        copy = remote(c_out.at[j], c_in.at[j], send.at[2, j], recv.at[2, j], "mp", other)
        copy.start()
        third.append(copy)
    for j in range(pieces):
        third[j].wait_recv()
        total[(1 - core) * pieces + j] = c_in[j].astype(jnp.float32)
    sums = total[0]
    dots = total[0] * nf[:, :LANES]
    for i in range(1, 2 * pieces):
        sums = sums + total[i]
        dots = dots + total[i] * nf[:, i * LANES : (i + 1) * LANES]
    mean = jnp.sum(sums, axis=-1, keepdims=True) / width
    dot = jnp.sum(dots, axis=-1, keepdims=True) / width
    scale = inv[...]
    for i in range(2 * pieces):
        here = slice(i * LANES, (i + 1) * LANES)
        term = (total[i] - mean - nf[:, here] * dot) * scale
        if last:
            term_ref[:, here] = term
        ub_ref[:, here] = (cb[:, here].astype(jnp.float32) + term).astype(jnp.bfloat16)
    for copy in first + second + third:
        copy.wait_send()


def reduce_norm(part, nf, inv, cb, last, ident):
    tokens, width = part.shape
    pieces = width // 2 // LANES
    shapes = [jax.ShapeDtypeStruct((tokens, width), jnp.bfloat16)]
    if last:
        shapes.append(jax.ShapeDtypeStruct((tokens, width), jnp.float32))
    wide = pltpu.VMEM((pieces, tokens, LANES), jnp.float32)
    slim = pltpu.VMEM((pieces, tokens, LANES), jnp.bfloat16)
    return pl.pallas_call(
        functools.partial(reduce_kernel, last),
        name="reduce_last" if last else "reduce_mid",
        out_shape=tuple(shapes),
        in_specs=vmem(4),
        out_specs=tuple(vmem(len(shapes))),
        scratch_shapes=[
            wide, wide, slim, slim, slim, slim,
            pltpu.VMEM((2 * pieces, tokens, LANES), jnp.float32),
            pltpu.SemaphoreType.DMA((3, pieces)),
            pltpu.SemaphoreType.DMA((3, pieces)),
        ],
        compiler_params=pltpu.CompilerParams(collective_id=ident, has_side_effects=True),
    )(part, nf, inv, cb)


def scatter_kernel(bits, chunks, factor, g_ref, out_ref, *scratch):
    send, recv = scratch[-2:]
    bufs = scratch[:-2]
    me = lax.axis_index("dp")
    mine = [lax.rem(me // (2**b), 2) for b in range(bits)]
    partner = [me + (2**b) * (1 - 2 * mine[b]) for b in range(bits)]
    greet("dp", partner)
    rows = g_ref.shape[-2] // chunks

    def pick(ref, left, b, value, extra):
        where = tuple(value if d == b else slice(None) for d in left)
        return ref.at[where + extra]

    state = []
    for j in range(chunks):
        order = list(range(bits))
        if j % 2 == 1 and bits > 1:
            order[0], order[1] = order[1], order[0]
        state.append(order)
    copies = {}

    def source(j, s):
        left = [d for d in reversed(range(bits)) if d not in state[j][:s]]
        if s == 0:
            return g_ref, left, (pl.ds(j * rows, rows),)
        return bufs[(s - 1) * 2 + 1].at[j], left, ()

    def begin(j, s):
        b = state[j][s]
        ref, left, extra = source(j, s)
        copy = remote(
            pick(ref, left, b, 1 - mine[b], extra), bufs[s * 2].at[j],
            send.at[s, j], recv.at[s, j], "dp", partner[b],
        )
        copy.start()
        copies[s, j] = copy

    def end(j, s):
        b = state[j][s]
        ref, left, extra = source(j, s)
        copies[s, j].wait_recv()
        kept = pick(ref, left, b, mine[b], extra)[...].astype(jnp.float32)
        summed = kept + bufs[s * 2][j].astype(jnp.float32)
        if s == bits - 1:
            out_ref[j * rows : (j + 1) * rows, :] = summed * factor
        else:
            bufs[s * 2 + 1][j] = summed.astype(jnp.bfloat16)
            begin(j, s + 1)

    for j in range(chunks):
        begin(j, 0)
    for step in range(chunks + bits - 1):
        for s in reversed(range(bits)):
            j = step - s
            if 0 <= j < chunks:
                end(j, s)
    for copy in copies.values():
        copy.wait_send()


def scatter(g, ranks, factor):
    bits = ranks.bit_length() - 1
    height, width = g.shape
    block = height // ranks
    chunks = 10 if block % 160 == 0 else 1
    rows = block // chunks
    scratch = []
    for s in range(bits):
        shape = (chunks,) + (2,) * (bits - 1 - s) + (rows, width)
        scratch.append(pltpu.VMEM(shape, jnp.bfloat16))
        scratch.append(pltpu.VMEM(shape, jnp.bfloat16))
    return pl.pallas_call(
        functools.partial(scatter_kernel, bits, chunks, factor),
        name="scatter_dp",
        out_shape=jax.ShapeDtypeStruct((block, width), jnp.float32),
        in_specs=vmem(1),
        out_specs=pl.BlockSpec(memory_space=pltpu.VMEM),
        scratch_shapes=scratch
        + [pltpu.SemaphoreType.DMA((bits, chunks)), pltpu.SemaphoreType.DMA((bits, chunks))],
        compiler_params=pltpu.CompilerParams(collective_id=3, has_side_effects=True),
    )(g.reshape((2,) * bits + (block, width)))


def shards(z_star, cotangent, w_qkv, w_out):
    ranks = lax.axis_size("dp")
    images, tokens, narrow = z_star.shape
    columns = w_qkv.shape[2]
    heads_here = columns // HD
    score_scale = HD ** (-0.5)
    position = lax.axis_index("mp")
    normal_f, flattened, inv_std, cot_rows = gather(z_star[0], cotangent[0])

    def project(slot_index):
        result = jnp.dot(flattened, w_qkv[slot_index], preferred_element_type=jnp.float32)
        return result.astype(jnp.bfloat16).reshape(images, tokens, heads_here, HD)

    queries = project(0)
    key_vecs = project(1)
    val_vecs = project(2)
    scores = (
        jnp.einsum("bqhe,bkhe->bhqk", queries, key_vecs, preferred_element_type=jnp.float32)
        * score_scale
    )
    attn_probs = jax.nn.softmax(scores, axis=-1)
    probs_b = attn_probs.astype(jnp.bfloat16)
    attended = jnp.einsum("bhqk,bkhe->bqhe", probs_b, val_vecs, preferred_element_type=jnp.float32)
    attended = attended.astype(jnp.bfloat16).reshape(-1, columns)
    contract_first = (((0,), (0,)), ((), ()))
    contract_second = (((1,), (1,)), ((), ()))

    def pull_back(rows):
        att_grad = lax.dot_general(rows, w_out, contract_second, preferred_element_type=jnp.float32)
        att_grad = att_grad.astype(jnp.bfloat16).reshape(images, tokens, heads_here, HD)
        prob_grad = jnp.einsum(
            "bqhe,bkhe->bhqk", att_grad, val_vecs, preferred_element_type=jnp.float32
        )
        rowdot = jnp.sum(attn_probs * prob_grad, axis=-1, keepdims=True)
        score_grad = (attn_probs * (prob_grad - rowdot) * score_scale).astype(jnp.bfloat16)
        q_grad = jnp.einsum(
            "bhqk,bkhe->bqhe", score_grad, key_vecs, preferred_element_type=jnp.float32
        ).astype(jnp.bfloat16)
        k_grad = jnp.einsum(
            "bhqk,bqhe->bkhe", score_grad, queries, preferred_element_type=jnp.float32
        ).astype(jnp.bfloat16)
        v_grad = jnp.einsum(
            "bhqk,bqhe->bkhe", probs_b, att_grad, preferred_element_type=jnp.float32
        ).astype(jnp.bfloat16)
        return [item.reshape(-1, columns) for item in (q_grad, k_grad, v_grad)]

    rows = cot_rows
    term = None
    for term_index in range(TERMS - 1):
        grads = pull_back(rows)
        in_part = sum(
            lax.dot_general(grads[c], w_qkv[c], contract_second, preferred_element_type=jnp.float32)
            for c in range(3)
        )
        last = term_index + 2 == TERMS
        made = reduce_norm(in_part, normal_f, inv_std, cot_rows, last, 1 + term_index)
        rows = made[0]
        if last:
            term = made[1]
    implicit = cotangent + lax.dynamic_slice_in_dim(term, position * narrow, narrow, 1)[None]
    grads = pull_back(rows)
    pieces = [
        lax.dot_general(flattened, item, contract_first, preferred_element_type=jnp.float32)
        for item in grads
    ] + [lax.dot_general(rows, attended, contract_first, preferred_element_type=jnp.float32)]
    g = jnp.concatenate([item.astype(jnp.bfloat16) for item in pieces], axis=1)
    factor = 1.0 / math.sqrt(images * ranks * tokens)
    block = scatter(g, ranks, factor)
    grad_qkv = jnp.stack([block[:, c * columns : (c + 1) * columns] for c in range(3)])
    grad_out = block[:, 3 * columns :].T
    return (implicit, grad_qkv, grad_out)


def solution(mesh):
    return jax.shard_map(
        shards,
        mesh=mesh,
        in_specs=(P("dp", None, "mp"), P("dp", None, "mp"), P(None, None, "mp"), P("mp", None)),
        out_specs=(P("dp", None, "mp"), P(None, "dp", "mp"), P("mp", "dp")),
        check_vma=False,
    )
```

```python
import functools
import math

import jax
import jax.numpy as jnp
from jax import lax
from jax.experimental import pallas as pl
from jax.experimental.pallas import tpu as pltpu
from jax.sharding import PartitionSpec as P

HD = 80
TERMS = 3
LANES = 128
MESH = pl.DeviceIdType.MESH


epsilon = 1e-06


def greet(axis, partners):
    barrier = pltpu.get_barrier_semaphore()
    for partner in partners:
        pl.semaphore_signal(barrier, inc=1, device_id={axis: partner}, device_id_type=MESH)
    pl.semaphore_wait(barrier, len(partners))


def remote(src, dst, send, recv, axis, target):
    return pltpu.make_async_remote_copy(
        src_ref=src, dst_ref=dst, send_sem=send, recv_sem=recv,
        device_id={axis: target}, device_id_type=MESH,
    )


def mp_partners():
    me = lax.axis_index("mp")
    core = lax.rem(me, 2)
    return me, core, me + 1 - 2 * core, lax.rem(me + 2, 4)


def gather_kernel(z_ref, cot_ref, nf_ref, nb_ref, inv_ref, cb_ref, cast, z_all, c_all, send, recv):
    me, core, other, across = mp_partners()
    narrow = z_ref.shape[1]
    cast[...] = cot_ref[...].astype(jnp.bfloat16)
    greet("mp", (other, across))
    copies = []
    for k, (src, held) in enumerate(((z_ref, z_all), (cast, c_all))):
        far = remote(src, held.at[me], send.at[k, 0], recv.at[k, 0], "mp", across)
        near = remote(src, held.at[me], send.at[k, 1], recv.at[k, 1], "mp", other)
        far.start()
        near.start()
        copies.append((far, near))

    def finish(k, src, held):
        far, near = copies[k]
        held[me] = src[...]
        far.wait_recv()
        passed = remote(
            held.at[across], held.at[across], send.at[k, 2], recv.at[k, 2], "mp", other
        )
        passed.start()
        near.wait_recv()
        passed.wait_recv()
        far.wait_send()
        near.wait_send()
        passed.wait_send()

    finish(0, z_ref, z_all)
    for s in range(4):
        nf_ref[:, s * narrow : (s + 1) * narrow] = z_all[s].astype(jnp.float32)
    values = nf_ref[...]
    centred = values - jnp.mean(values, axis=-1, keepdims=True)
    inv = lax.rsqrt(jnp.mean(centred * centred, axis=-1, keepdims=True) + epsilon)
    normal = centred * inv
    nf_ref[...] = normal
    nb_ref[...] = normal.astype(jnp.bfloat16)
    inv_ref[...] = inv
    finish(1, cast, c_all)
    for s in range(4):
        cb_ref[:, s * narrow : (s + 1) * narrow] = c_all[s]


def vmem(count):
    return [pl.BlockSpec(memory_space=pltpu.VMEM)] * count


def gather(z, cot):
    tokens, narrow = z.shape
    width = narrow * 4
    held = pltpu.VMEM((4, tokens, narrow), jnp.bfloat16)
    return pl.pallas_call(
        gather_kernel,
        name="gather_mp",
        out_shape=(
            jax.ShapeDtypeStruct((tokens, width), jnp.float32),
            jax.ShapeDtypeStruct((tokens, width), jnp.bfloat16),
            jax.ShapeDtypeStruct((tokens, 1), jnp.float32),
            jax.ShapeDtypeStruct((tokens, width), jnp.bfloat16),
        ),
        in_specs=vmem(2),
        out_specs=tuple(vmem(4)),
        scratch_shapes=[
            pltpu.VMEM((tokens, narrow), jnp.bfloat16),
            held,
            held,
            pltpu.SemaphoreType.DMA((2, 3)),
            pltpu.SemaphoreType.DMA((2, 3)),
        ],
        compiler_params=pltpu.CompilerParams(collective_id=0, has_side_effects=True),
    )(z, cot)


def reduce_kernel(last, part, nf, inv, cb, *refs):
    if last:
        cot, ub_ref, out_ref, a_in, acc, b_out, b_in, c_out, c_in, total, term_ref, send, recv = refs
    else:
        ub_ref, a_in, acc, b_out, b_in, c_out, c_in, total, send, recv = refs
    me, core, other, across = mp_partners()
    width = part.shape[1]
    half = width // 2
    pieces = half // LANES
    greet("mp", (other, across))

    def columns(which, j):
        return pl.ds(pl.multiple_of(which * half + j * LANES, LANES), LANES)

    first, second, third = [], [], []
    for j in range(pieces):
        copy = remote(
            part.at[:, columns(1 - core, j)], a_in.at[j], send.at[0, j], recv.at[0, j], "mp", other
        )
        copy.start()
        first.append(copy)
    for j in range(pieces):
        first[j].wait_recv()
        summed = part[:, columns(core, j)] + a_in[j]
        acc[j] = summed
        b_out[j] = summed.astype(jnp.bfloat16)
        copy = remote(b_out.at[j], b_in.at[j], send.at[1, j], recv.at[1, j], "mp", across)
        copy.start()
        second.append(copy)
    for j in range(pieces):
        second[j].wait_recv()
        summed = acc[j] + b_in[j].astype(jnp.float32)
        total[core * pieces + j] = summed
        c_out[j] = summed.astype(jnp.bfloat16)
        copy = remote(c_out.at[j], c_in.at[j], send.at[2, j], recv.at[2, j], "mp", other)
        copy.start()
        third.append(copy)
    for j in range(pieces):
        third[j].wait_recv()
        total[(1 - core) * pieces + j] = c_in[j].astype(jnp.float32)
    sums = total[0]
    dots = total[0] * nf[:, :LANES]
    for i in range(1, 2 * pieces):
        sums = sums + total[i]
        dots = dots + total[i] * nf[:, i * LANES : (i + 1) * LANES]
    mean = jnp.sum(sums, axis=-1, keepdims=True) / width
    dot = jnp.sum(dots, axis=-1, keepdims=True) / width
    scale = inv[...]
    for i in range(2 * pieces):
        here = slice(i * LANES, (i + 1) * LANES)
        term = (total[i] - mean - nf[:, here] * dot) * scale
        if last:
            term_ref[:, here] = term
        ub_ref[:, here] = (cb[:, here].astype(jnp.float32) + term).astype(jnp.bfloat16)
    if last:
        narrow = out_ref.shape[1]
        for s in range(4):

            @pl.when(me == s)
            def _(s=s):
                out_ref[...] = cot[...] + term_ref[:, s * narrow : (s + 1) * narrow]

    for copy in first + second + third:
        copy.wait_send()


def reduce_norm(part, nf, inv, cb, cot, last, ident):
    tokens, width = part.shape
    pieces = width // 2 // LANES
    shapes = [jax.ShapeDtypeStruct((tokens, width), jnp.bfloat16)]
    if last:
        shapes.append(jax.ShapeDtypeStruct(cot.shape, jnp.float32))
    wide = pltpu.VMEM((pieces, tokens, LANES), jnp.float32)
    slim = pltpu.VMEM((pieces, tokens, LANES), jnp.bfloat16)
    return pl.pallas_call(
        functools.partial(reduce_kernel, last),
        name="reduce_last" if last else "reduce_mid",
        out_shape=tuple(shapes),
        in_specs=vmem(5 if last else 4),
        out_specs=tuple(vmem(len(shapes))),
        scratch_shapes=[
            wide, wide, slim, slim, slim, slim,
            pltpu.VMEM((2 * pieces, tokens, LANES), jnp.float32),
        ]
        + ([pltpu.VMEM((tokens, width), jnp.float32)] if last else [])
        + [
            pltpu.SemaphoreType.DMA((3, pieces)),
            pltpu.SemaphoreType.DMA((3, pieces)),
        ],
        compiler_params=pltpu.CompilerParams(collective_id=ident, has_side_effects=True),
    )(*((part, nf, inv, cb, cot) if last else (part, nf, inv, cb)))


def scatter_kernel(bits, chunks, factor, g_ref, out_ref, *scratch):
    send, recv = scratch[-2:]
    bufs = scratch[:-2]
    me = lax.axis_index("dp")
    mine = [lax.rem(me // (2**b), 2) for b in range(bits)]
    partner = [me + (2**b) * (1 - 2 * mine[b]) for b in range(bits)]
    greet("dp", partner)
    rows = g_ref.shape[-2] // chunks

    def pick(ref, left, b, value, extra):
        where = tuple(value if d == b else slice(None) for d in left)
        return ref.at[where + extra]

    state = []
    for j in range(chunks):
        order = list(range(bits))
        if j % 2 == 1 and bits > 1:
            order[0], order[1] = order[1], order[0]
        state.append(order)
    copies = {}

    def source(j, s):
        left = [d for d in reversed(range(bits)) if d not in state[j][:s]]
        if s == 0:
            return g_ref, left, (pl.ds(j * rows, rows),)
        return bufs[(s - 1) * 2 + 1].at[j], left, ()

    def begin(j, s):
        b = state[j][s]
        ref, left, extra = source(j, s)
        copy = remote(
            pick(ref, left, b, 1 - mine[b], extra), bufs[s * 2].at[j],
            send.at[s, j], recv.at[s, j], "dp", partner[b],
        )
        copy.start()
        copies[s, j] = copy

    def end(j, s):
        b = state[j][s]
        ref, left, extra = source(j, s)
        copies[s, j].wait_recv()
        kept = pick(ref, left, b, mine[b], extra)[...].astype(jnp.float32)
        summed = kept + bufs[s * 2][j].astype(jnp.float32)
        if s == bits - 1:
            out_ref[j * rows : (j + 1) * rows, :] = summed * factor
        else:
            bufs[s * 2 + 1][j] = summed.astype(jnp.bfloat16)
            begin(j, s + 1)

    for j in range(chunks):
        begin(j, 0)
    for step in range(chunks + bits - 1):
        for s in reversed(range(bits)):
            j = step - s
            if 0 <= j < chunks:
                end(j, s)
    for copy in copies.values():
        copy.wait_send()


def scatter(g, ranks, factor):
    bits = ranks.bit_length() - 1
    height, width = g.shape
    block = height // ranks
    chunks = 5 if block % 160 == 0 else 1
    rows = block // chunks
    scratch = []
    for s in range(bits):
        shape = (chunks,) + (2,) * (bits - 1 - s) + (rows, width)
        scratch.append(pltpu.VMEM(shape, jnp.bfloat16))
        scratch.append(pltpu.VMEM(shape, jnp.bfloat16))
    return pl.pallas_call(
        functools.partial(scatter_kernel, bits, chunks, factor),
        name="scatter_dp",
        out_shape=jax.ShapeDtypeStruct((block, width), jnp.float32),
        in_specs=vmem(1),
        out_specs=pl.BlockSpec(memory_space=pltpu.VMEM),
        scratch_shapes=scratch
        + [pltpu.SemaphoreType.DMA((bits, chunks)), pltpu.SemaphoreType.DMA((bits, chunks))],
        compiler_params=pltpu.CompilerParams(collective_id=3, has_side_effects=True),
    )(g.reshape((2,) * bits + (block, width)))


def dot_nt(a, b):
    return lax.dot_general(a, b, (((1,), (1,)), ((), ())), preferred_element_type=jnp.float32)


def dot_tn(a, b):
    return lax.dot_general(a, b, (((0,), (0,)), ((), ())), preferred_element_type=jnp.float32)


def windows(columns):
    for h in range(columns // HD):
        low = h * HD // LANES * LANES
        high = min(-(-(h + 1) * HD // LANES) * LANES, columns)
        yield h, slice(low, high), h * HD - low


def only_head(value, start):
    lane = lax.broadcasted_iota(jnp.int32, value.shape, 1)
    return jnp.where((lane >= start) & (lane < start + HD), value, jnp.zeros_like(value))


def forward_step(nb, w, q, k, v, probs, att, hold):
    scale = HD ** (-0.5)
    normal = nb[...]
    for c, ref in enumerate((q, k, v)):
        made = jnp.dot(normal, w[c], preferred_element_type=jnp.float32)
        ref[...] = made.astype(jnp.bfloat16)
    hold[...] = jnp.zeros_like(hold)
    for h, here, start in windows(q.shape[1]):
        scores = dot_nt(only_head(q[:, here], start), k[:, here]) * scale
        raised = jnp.exp(scores - jnp.max(scores, axis=-1, keepdims=True))
        share = raised / jnp.sum(raised, axis=-1, keepdims=True)
        probs[h] = share
        hold[:, here] += jnp.dot(
            share.astype(jnp.bfloat16),
            only_head(v[:, here], start),
            preferred_element_type=jnp.float32,
        )
    att[...] = hold[...].astype(jnp.bfloat16)


def pull_step(rows, wo, q, k, v, probs, holds):
    scale = HD ** (-0.5)
    grad = dot_nt(rows[...], wo[...]).astype(jnp.bfloat16)
    for ref in holds:
        ref[...] = jnp.zeros_like(ref)
    for h, here, start in windows(q.shape[1]):
        own = only_head(grad[:, here], start)
        pg = dot_nt(own, v[:, here])
        share = probs[h]
        rowdot = jnp.sum(share * pg, axis=-1, keepdims=True)
        sg = (share * (pg - rowdot) * scale).astype(jnp.bfloat16)
        holds[0][:, here] += jnp.dot(
            sg, only_head(k[:, here], start), preferred_element_type=jnp.float32
        )
        holds[1][:, here] += dot_tn(sg, only_head(q[:, here], start))
        holds[2][:, here] += dot_tn(share.astype(jnp.bfloat16), own)
    return [ref[...].astype(jnp.bfloat16) for ref in holds]


def back_to_input(grads, w, part):
    part[...] = dot_nt(grads[0], w[0])
    part[...] += dot_nt(grads[1], w[1])
    part[...] += dot_nt(grads[2], w[2])


def first_kernel(nb, rows, w, wo, q, k, v, probs, att, part, *holds):
    forward_step(nb, w, q, k, v, probs, att, holds[0])
    back_to_input(pull_step(rows, wo, q, k, v, probs, holds), w, part)


def middle_kernel(rows, w, wo, q, k, v, probs, part, *holds):
    back_to_input(pull_step(rows, wo, q, k, v, probs, holds), w, part)


def final_kernel(rows, nb, wo, q, k, v, probs, att, g, *holds):
    side = holds[3]
    grads = pull_step(rows, wo, q, k, v, probs, holds[:3])
    columns = q.shape[1]
    for c, item in enumerate(grads + [att[...]]):
        side[:, c * columns : (c + 1) * columns] = item
    cut = 3 * columns
    low, high = cut // LANES * LANES, -(-cut // LANES) * LANES
    height = g.shape[0]
    step = 256 if height % 256 == 0 else height
    for i in range(height // step):
        here = slice(i * step, (i + 1) * step)
        left = dot_tn(nb[:, here], side[:, :high])
        right = dot_tn(rows[:, here], side[:, low:])
        g[here, :low] = left[:, :low].astype(jnp.bfloat16)
        if high > low:
            lane = lax.broadcasted_iota(jnp.int32, (step, high - low), 1)
            mixed = jnp.where(lane < cut - low, left[:, low:], right[:, : high - low])
            g[here, low:high] = mixed.astype(jnp.bfloat16)
        g[here, high:] = right[:, high - low :].astype(jnp.bfloat16)


def local(body, name, shapes, arrays, scratch, flops):
    return pl.pallas_call(
        body,
        name=name,
        out_shape=tuple(shapes),
        in_specs=vmem(len(arrays)),
        out_specs=tuple(vmem(len(shapes))),
        scratch_shapes=scratch,
        cost_estimate=pl.CostEstimate(flops=flops, bytes_accessed=4 << 20, transcendentals=0),
    )(*arrays)


def shards(z_star, cotangent, w_qkv, w_out):
    ranks = lax.axis_size("dp")
    images, tokens, narrow = z_star.shape
    columns = w_qkv.shape[2]
    width = w_qkv.shape[1]
    heads_here = columns // HD
    normal_f, normal_b, inv_std, cot_rows = gather(z_star[0], cotangent[0])
    flat = jax.ShapeDtypeStruct((tokens, columns), jnp.bfloat16)
    wide = jax.ShapeDtypeStruct((tokens, width), jnp.float32)
    shares = jax.ShapeDtypeStruct((heads_here, tokens, tokens), jnp.float32)
    holds = [pltpu.VMEM((tokens, columns), jnp.float32)] * 3
    work = 6 * tokens * width * columns
    q, k, v, probs, att, part = local(
        first_kernel, "first", (flat, flat, flat, shares, flat, wide),
        (normal_b, cot_rows, w_qkv, w_out), holds, 3 * work,
    )
    rows = cot_rows
    for term_index in range(TERMS - 1):
        if term_index:
            (part,) = local(
                middle_kernel, "middle", (wide,), (rows, w_qkv, w_out, q, k, v, probs), holds, 2 * work
            )
        last = term_index + 2 == TERMS
        made = reduce_norm(part, normal_f, inv_std, cot_rows, cotangent[0], last, 1 + term_index)
        rows = made[0]
    implicit = made[1][None]
    (g,) = local(
        final_kernel, "final", (jax.ShapeDtypeStruct((width, 4 * columns), jnp.bfloat16),),
        (rows, normal_b, w_out, q, k, v, probs, att),
        holds + [pltpu.VMEM((tokens, 4 * columns), jnp.bfloat16)], 2 * work,
    )
    factor = 1.0 / math.sqrt(images * ranks * tokens)
    block = scatter(g, ranks, factor)
    grad_qkv = jnp.stack([block[:, c * columns : (c + 1) * columns] for c in range(3)])
    grad_out = block[:, 3 * columns :].T
    return (implicit, grad_qkv, grad_out)


def solution(mesh):
    return jax.shard_map(
        shards,
        mesh=mesh,
        in_specs=(P("dp", None, "mp"), P("dp", None, "mp"), P(None, None, "mp"), P("mp", None)),
        out_specs=(P("dp", None, "mp"), P(None, "dp", "mp"), P("mp", "dp")),
        check_vma=False,
    )
```

```python
import functools
import math

import jax
import jax.numpy as jnp
from jax import lax
from jax.experimental import pallas as pl
from jax.experimental.pallas import tpu as pltpu
from jax.sharding import PartitionSpec as P

HD = 80
TERMS = 3
LANES = 128
MESH = pl.DeviceIdType.MESH


epsilon = 1e-06


def greet(axis, partners):
    barrier = pltpu.get_barrier_semaphore()
    for partner in partners:
        pl.semaphore_signal(barrier, inc=1, device_id={axis: partner}, device_id_type=MESH)
    pl.semaphore_wait(barrier, len(partners))


def remote(src, dst, send, recv, axis, target):
    return pltpu.make_async_remote_copy(
        src_ref=src, dst_ref=dst, send_sem=send, recv_sem=recv,
        device_id={axis: target}, device_id_type=MESH,
    )


def mp_partners():
    me = lax.axis_index("mp")
    core = lax.rem(me, 2)
    return me, core, me + 1 - 2 * core, lax.rem(me + 2, 4)


def gather_kernel(z_ref, cot_ref, nf_ref, nb_ref, inv_ref, cb_ref, cast, z_all, c_all, send, recv):
    me, core, other, across = mp_partners()
    narrow = z_ref.shape[1]
    cast[...] = cot_ref[...].astype(jnp.bfloat16)
    greet("mp", (other, across))
    copies = []
    for k, (src, held) in enumerate(((z_ref, z_all), (cast, c_all))):
        far = remote(src, held.at[me], send.at[k, 0], recv.at[k, 0], "mp", across)
        near = remote(src, held.at[me], send.at[k, 1], recv.at[k, 1], "mp", other)
        far.start()
        near.start()
        copies.append((far, near))

    def finish(k, src, held):
        far, near = copies[k]
        held[me] = src[...]
        far.wait_recv()
        passed = remote(
            held.at[across], held.at[across], send.at[k, 2], recv.at[k, 2], "mp", other
        )
        passed.start()
        near.wait_recv()
        passed.wait_recv()
        far.wait_send()
        near.wait_send()
        passed.wait_send()

    finish(0, z_ref, z_all)
    for s in range(4):
        nf_ref[:, s * narrow : (s + 1) * narrow] = z_all[s].astype(jnp.float32)
    values = nf_ref[...]
    centred = values - jnp.mean(values, axis=-1, keepdims=True)
    inv = lax.rsqrt(jnp.mean(centred * centred, axis=-1, keepdims=True) + epsilon)
    normal = centred * inv
    nf_ref[...] = normal
    nb_ref[...] = normal.astype(jnp.bfloat16)
    inv_ref[...] = inv
    finish(1, cast, c_all)
    for s in range(4):
        cb_ref[:, s * narrow : (s + 1) * narrow] = c_all[s]


def vmem(count):
    return [pl.BlockSpec(memory_space=pltpu.VMEM)] * count


def gather(z, cot):
    tokens, narrow = z.shape
    width = narrow * 4
    held = pltpu.VMEM((4, tokens, narrow), jnp.bfloat16)
    return pl.pallas_call(
        gather_kernel,
        name="gather_mp",
        out_shape=(
            jax.ShapeDtypeStruct((tokens, width), jnp.float32),
            jax.ShapeDtypeStruct((tokens, width), jnp.bfloat16),
            jax.ShapeDtypeStruct((tokens, 1), jnp.float32),
            jax.ShapeDtypeStruct((tokens, width), jnp.bfloat16),
        ),
        in_specs=vmem(2),
        out_specs=tuple(vmem(4)),
        scratch_shapes=[
            pltpu.VMEM((tokens, narrow), jnp.bfloat16),
            held,
            held,
            pltpu.SemaphoreType.DMA((2, 3)),
            pltpu.SemaphoreType.DMA((2, 3)),
        ],
        compiler_params=pltpu.CompilerParams(collective_id=0, has_side_effects=True),
    )(z, cot)


def reduce_kernel(last, part, nf, inv, cb, *refs):
    if last:
        cot, ub_ref, out_ref, a_in, acc, b_out, b_in, c_out, c_in, total, term_ref, send, recv = refs
    else:
        ub_ref, a_in, acc, b_out, b_in, c_out, c_in, total, send, recv = refs
    me, core, other, across = mp_partners()
    width = part.shape[1]
    half = width // 2
    pieces = half // LANES
    greet("mp", (other, across))

    def columns(which, j):
        return pl.ds(pl.multiple_of(which * half + j * LANES, LANES), LANES)

    first, second, third = [], [], []
    for j in range(pieces):
        copy = remote(
            part.at[:, columns(1 - core, j)], a_in.at[j], send.at[0, j], recv.at[0, j], "mp", other
        )
        copy.start()
        first.append(copy)
    for j in range(pieces):
        first[j].wait_recv()
        summed = part[:, columns(core, j)] + a_in[j]
        acc[j] = summed
        b_out[j] = summed.astype(jnp.bfloat16)
        copy = remote(b_out.at[j], b_in.at[j], send.at[1, j], recv.at[1, j], "mp", across)
        copy.start()
        second.append(copy)
    for j in range(pieces):
        second[j].wait_recv()
        summed = acc[j] + b_in[j].astype(jnp.float32)
        total[core * pieces + j] = summed
        c_out[j] = summed.astype(jnp.bfloat16)
        copy = remote(c_out.at[j], c_in.at[j], send.at[2, j], recv.at[2, j], "mp", other)
        copy.start()
        third.append(copy)
    for j in range(pieces):
        third[j].wait_recv()
        total[(1 - core) * pieces + j] = c_in[j].astype(jnp.float32)
    sums = total[0]
    dots = total[0] * nf[:, :LANES]
    for i in range(1, 2 * pieces):
        sums = sums + total[i]
        dots = dots + total[i] * nf[:, i * LANES : (i + 1) * LANES]
    mean = jnp.sum(sums, axis=-1, keepdims=True) / width
    dot = jnp.sum(dots, axis=-1, keepdims=True) / width
    scale = inv[...]
    for i in range(2 * pieces):
        here = slice(i * LANES, (i + 1) * LANES)
        term = (total[i] - mean - nf[:, here] * dot) * scale
        if last:
            term_ref[:, here] = term
        ub_ref[:, here] = (cb[:, here].astype(jnp.float32) + term).astype(jnp.bfloat16)
    if last:
        narrow = out_ref.shape[1]
        for s in range(4):

            @pl.when(me == s)
            def _(s=s):
                out_ref[...] = cot[...] + term_ref[:, s * narrow : (s + 1) * narrow]

    for copy in first + second + third:
        copy.wait_send()


def reduce_norm(part, nf, inv, cb, cot, last, ident):
    tokens, width = part.shape
    pieces = width // 2 // LANES
    shapes = [jax.ShapeDtypeStruct((tokens, width), jnp.bfloat16)]
    if last:
        shapes.append(jax.ShapeDtypeStruct(cot.shape, jnp.float32))
    wide = pltpu.VMEM((pieces, tokens, LANES), jnp.float32)
    slim = pltpu.VMEM((pieces, tokens, LANES), jnp.bfloat16)
    return pl.pallas_call(
        functools.partial(reduce_kernel, last),
        name="reduce_last" if last else "reduce_mid",
        out_shape=tuple(shapes),
        in_specs=vmem(5 if last else 4),
        out_specs=tuple(vmem(len(shapes))),
        scratch_shapes=[
            wide, wide, slim, slim, slim, slim,
            pltpu.VMEM((2 * pieces, tokens, LANES), jnp.float32),
        ]
        + ([pltpu.VMEM((tokens, width), jnp.float32)] if last else [])
        + [
            pltpu.SemaphoreType.DMA((3, pieces)),
            pltpu.SemaphoreType.DMA((3, pieces)),
        ],
        compiler_params=pltpu.CompilerParams(collective_id=ident, has_side_effects=True),
    )(*((part, nf, inv, cb, cot) if last else (part, nf, inv, cb)))


def scatter_kernel(bits, chunks, factor, g_ref, qkv_ref, out_ref, *scratch):
    send, recv = scratch[-2:]
    bufs = scratch[:-2]
    me = lax.axis_index("dp")
    mine = [lax.rem(me // (2**b), 2) for b in range(bits)]
    partner = [me + (2**b) * (1 - 2 * mine[b]) for b in range(bits)]
    greet("dp", partner)
    rows = g_ref.shape[-2] // chunks

    def pick(ref, left, b, value, extra):
        where = tuple(value if d == b else slice(None) for d in left)
        return ref.at[where + extra]

    state = []
    for j in range(chunks):
        order = list(range(bits))
        if j % 2 == 1 and bits > 1:
            order[0], order[1] = order[1], order[0]
        state.append(order)
    copies = {}

    def source(j, s):
        left = [d for d in reversed(range(bits)) if d not in state[j][:s]]
        if s == 0:
            return g_ref, left, (pl.ds(j * rows, rows),)
        return bufs[(s - 1) * 2 + 1].at[j], left, ()

    def begin(j, s):
        b = state[j][s]
        ref, left, extra = source(j, s)
        copy = remote(
            pick(ref, left, b, 1 - mine[b], extra), bufs[s * 2].at[j],
            send.at[s, j], recv.at[s, j], "dp", partner[b],
        )
        copy.start()
        copies[s, j] = copy

    def end(j, s):
        b = state[j][s]
        ref, left, extra = source(j, s)
        copies[s, j].wait_recv()
        kept = pick(ref, left, b, mine[b], extra)[...].astype(jnp.float32)
        summed = kept + bufs[s * 2][j].astype(jnp.float32)
        if s == bits - 1:
            here = slice(j * rows, (j + 1) * rows)
            columns = out_ref.shape[1]
            scaled = summed * factor
            for c in range(3):
                qkv_ref[c, here, :] = scaled[:, c * columns : (c + 1) * columns]
            out_ref[here, :] = scaled[:, 3 * columns :]
        else:
            bufs[s * 2 + 1][j] = summed.astype(jnp.bfloat16)
            begin(j, s + 1)

    for j in range(chunks):
        begin(j, 0)
    for step in range(chunks + bits - 1):
        for s in reversed(range(bits)):
            j = step - s
            if 0 <= j < chunks:
                end(j, s)
    for copy in copies.values():
        copy.wait_send()


def scatter(g, ranks, factor):
    bits = ranks.bit_length() - 1
    height, width = g.shape
    block = height // ranks
    chunks = 5 if block % 160 == 0 else 1
    rows = block // chunks
    scratch = []
    for s in range(bits):
        shape = (chunks,) + (2,) * (bits - 1 - s) + (rows, width)
        scratch.append(pltpu.VMEM(shape, jnp.bfloat16))
        scratch.append(pltpu.VMEM(shape, jnp.bfloat16))
    return pl.pallas_call(
        functools.partial(scatter_kernel, bits, chunks, factor),
        name="scatter_dp",
        out_shape=(
            jax.ShapeDtypeStruct((3, block, width // 4), jnp.float32),
            jax.ShapeDtypeStruct((block, width // 4), jnp.float32),
        ),
        in_specs=vmem(1),
        out_specs=tuple(vmem(2)),
        scratch_shapes=scratch
        + [pltpu.SemaphoreType.DMA((bits, chunks)), pltpu.SemaphoreType.DMA((bits, chunks))],
        compiler_params=pltpu.CompilerParams(collective_id=3, has_side_effects=True),
    )(g.reshape((2,) * bits + (block, width)))


def dot_nt(a, b):
    return lax.dot_general(a, b, (((1,), (1,)), ((), ())), preferred_element_type=jnp.float32)


def dot_tn(a, b):
    return lax.dot_general(a, b, (((0,), (0,)), ((), ())), preferred_element_type=jnp.float32)


def windows(columns):
    for h in range(columns // HD):
        low = h * HD // LANES * LANES
        high = min(-(-(h + 1) * HD // LANES) * LANES, columns)
        yield h, slice(low, high), h * HD - low


def only_head(value, start):
    lane = lax.broadcasted_iota(jnp.int32, value.shape, 1)
    return jnp.where((lane >= start) & (lane < start + HD), value, jnp.zeros_like(value))


def forward_step(nb, w, q, k, v, probs, att, hold):
    scale = HD ** (-0.5)
    normal = nb[...]
    for c, ref in enumerate((q, k, v)):
        made = dot_nt(normal, w[c])
        ref[...] = made.astype(jnp.bfloat16)
    hold[...] = jnp.zeros_like(hold)
    for h, here, start in windows(q.shape[1]):
        scores = dot_nt(only_head(q[:, here], start), k[:, here]) * scale
        raised = jnp.exp(scores - jnp.max(scores, axis=-1, keepdims=True))
        share = raised / jnp.sum(raised, axis=-1, keepdims=True)
        probs[h] = share
        hold[:, here] += jnp.dot(
            share.astype(jnp.bfloat16),
            only_head(v[:, here], start),
            preferred_element_type=jnp.float32,
        )
    att[...] = hold[...].astype(jnp.bfloat16)


def pull_step(rows, wo, q, k, v, probs, holds):
    scale = HD ** (-0.5)
    grad = dot_nt(rows[...], wo[...]).astype(jnp.bfloat16)
    for ref in holds:
        ref[...] = jnp.zeros_like(ref)
    for h, here, start in windows(q.shape[1]):
        own = only_head(grad[:, here], start)
        pg = dot_nt(own, v[:, here])
        share = probs[h]
        rowdot = jnp.sum(share * pg, axis=-1, keepdims=True)
        sg = (share * (pg - rowdot) * scale).astype(jnp.bfloat16)
        holds[0][:, here] += jnp.dot(
            sg, only_head(k[:, here], start), preferred_element_type=jnp.float32
        )
        holds[1][:, here] += dot_tn(sg, only_head(q[:, here], start))
        holds[2][:, here] += dot_tn(share.astype(jnp.bfloat16), own)
    return [ref[...].astype(jnp.bfloat16) for ref in holds]


def back_to_input(grads, w, part):
    part[...] = jnp.dot(grads[0], w[0], preferred_element_type=jnp.float32)
    part[...] += jnp.dot(grads[1], w[1], preferred_element_type=jnp.float32)
    part[...] += jnp.dot(grads[2], w[2], preferred_element_type=jnp.float32)


def first_kernel(nb, rows, w, wo, q, k, v, probs, att, part, *holds):
    forward_step(nb, w, q, k, v, probs, att, holds[0])
    back_to_input(pull_step(rows, wo, q, k, v, probs, holds), w, part)


def middle_kernel(rows, w, wo, q, k, v, probs, part, *holds):
    back_to_input(pull_step(rows, wo, q, k, v, probs, holds), w, part)


def final_kernel(rows, nb, wo, q, k, v, probs, att, g, *holds):
    side = holds[3]
    grads = pull_step(rows, wo, q, k, v, probs, holds[:3])
    columns = q.shape[1]
    for c, item in enumerate(grads + [att[...]]):
        side[:, c * columns : (c + 1) * columns] = item
    cut = 3 * columns
    low, high = cut // LANES * LANES, -(-cut // LANES) * LANES
    height = g.shape[0]
    step = 256 if height % 256 == 0 else height
    for i in range(height // step):
        here = slice(i * step, (i + 1) * step)
        left = dot_tn(nb[:, here], side[:, :high])
        right = dot_tn(rows[:, here], side[:, low:])
        g[here, :low] = left[:, :low].astype(jnp.bfloat16)
        if high > low:
            lane = lax.broadcasted_iota(jnp.int32, (step, high - low), 1)
            mixed = jnp.where(lane < cut - low, left[:, low:], right[:, : high - low])
            g[here, low:high] = mixed.astype(jnp.bfloat16)
        g[here, high:] = right[:, high - low :].astype(jnp.bfloat16)


def local(body, name, shapes, arrays, scratch, flops):
    return pl.pallas_call(
        body,
        name=name,
        out_shape=tuple(shapes),
        in_specs=vmem(len(arrays)),
        out_specs=tuple(vmem(len(shapes))),
        scratch_shapes=scratch,
        cost_estimate=pl.CostEstimate(flops=flops, bytes_accessed=4 << 20, transcendentals=0),
    )(*arrays)


def shards(z_star, cotangent, w_qkv, w_out):
    ranks = lax.axis_size("dp")
    images, tokens, narrow = z_star.shape
    columns = w_qkv.shape[2]
    width = w_qkv.shape[1]
    heads_here = columns // HD
    w_rows = jnp.swapaxes(w_qkv, 1, 2)
    normal_f, normal_b, inv_std, cot_rows = gather(z_star[0], cotangent[0])
    flat = jax.ShapeDtypeStruct((tokens, columns), jnp.bfloat16)
    wide = jax.ShapeDtypeStruct((tokens, width), jnp.float32)
    shares = jax.ShapeDtypeStruct((heads_here, tokens, tokens), jnp.float32)
    holds = [pltpu.VMEM((tokens, columns), jnp.float32)] * 3
    work = 6 * tokens * width * columns
    q, k, v, probs, att, part = local(
        first_kernel, "first", (flat, flat, flat, shares, flat, wide),
        (normal_b, cot_rows, w_rows, w_out), holds, 3 * work,
    )
    rows = cot_rows
    for term_index in range(TERMS - 1):
        if term_index:
            (part,) = local(
                middle_kernel, "middle", (wide,), (rows, w_rows, w_out, q, k, v, probs), holds, 2 * work
            )
        last = term_index + 2 == TERMS
        made = reduce_norm(part, normal_f, inv_std, cot_rows, cotangent[0], last, 1 + term_index)
        rows = made[0]
    implicit = made[1][None]
    (g,) = local(
        final_kernel, "final", (jax.ShapeDtypeStruct((width, 4 * columns), jnp.bfloat16),),
        (rows, normal_b, w_out, q, k, v, probs, att),
        holds + [pltpu.VMEM((tokens, 4 * columns), jnp.bfloat16)], 2 * work,
    )
    factor = 1.0 / math.sqrt(images * ranks * tokens)
    grad_qkv, turned = scatter(g, ranks, factor)
    grad_out = turned.T
    return (implicit, grad_qkv, grad_out)


def solution(mesh):
    return jax.shard_map(
        shards,
        mesh=mesh,
        in_specs=(P("dp", None, "mp"), P("dp", None, "mp"), P(None, None, "mp"), P("mp", None)),
        out_specs=(P("dp", None, "mp"), P(None, "dp", "mp"), P("mp", "dp")),
        check_vma=False,
    )
```
